16 devices in a mesh: dp: 1, sp: 16 (over x, y, z, core).
Axes of the slice: x: 2, y: 2, z: 2, core: 2. Of those that a mesh axis runs over, the one named last changes fastest.
Arguments:
- x: bfloat16 [8192, 2048], P(('dp', 'sp'))
- gain: bfloat16 [2048], replicated
- wq: bfloat16 [2048, 2048], P('sp')
- wk: bfloat16 [2048, 256], P('sp')
- wv: bfloat16 [2048, 256], P('sp')
- wo: bfloat16 [2048, 2048], P('sp')
Outputs:
- output: bfloat16 [8192, 2048], P(('dp', 'sp'))
All inputs are finite; a program needn't handle non-finite values.
Results may differ from the reference program's by a relative error of at most 0.012.
Values are sent between devices in bfloat16 or wider.
A program may use at most 2 GiB of HBM per device.

```python
import jax
import jax.numpy as jnp
from jax import lax

ROWS = 8192
D = 2048
HEADS = 8
KV_HEADS = 1
HEAD = 256
THETA = 10000


def setup_inputs(seed: int = 0, part: int = 0) -> dict:
    kx, kn, kq, kk, kv, ko = jax.random.split(jax.random.key(seed), 6)

    def weights(key, rows, columns):
        return jax.random.normal(key, (rows, columns), jnp.float32) * rows**-0.5

    drawn = {
        "x": jax.random.normal(jax.random.fold_in(kx, part), (ROWS, D), jnp.float32),
        "gain": 1 + 0.1 * jax.random.normal(kn, (D,), jnp.float32),
        "wq": 2 * weights(kq, D, HEADS * HEAD),
        "wk": 2 * weights(kk, D, KV_HEADS * HEAD),
        "wv": 4 * weights(kv, D, KV_HEADS * HEAD),
        "wo": weights(ko, HEADS * HEAD, D),
    }
    return {k: v.astype(jnp.bfloat16) for k, v in drawn.items()}


def normed(x, gain):
    wide = x.astype(jnp.float32)
    scale = lax.rsqrt(jnp.mean(wide * wide, -1, keepdims=True) + 1e-6)
    return (wide * scale * gain.astype(jnp.float32)).astype(jnp.bfloat16)


def turned(t, place, theta):
    half = t.shape[-1] // 2
    angle = place.astype(jnp.float32)[:, None] * theta ** (-jnp.arange(half, dtype=jnp.float32) / half)
    cos, sin = jnp.cos(angle)[:, None], jnp.sin(angle)[:, None]
    a, b = t[..., :half].astype(jnp.float32), t[..., half:].astype(jnp.float32)
    return jnp.concatenate([a * cos - b * sin, b * cos + a * sin], -1).astype(jnp.bfloat16)


def matmul(a, w):
    return jnp.dot(a, w, preferred_element_type=jnp.float32).astype(jnp.bfloat16)


def einsum(form, a, b):
    return jnp.einsum(form, a.astype(jnp.float32), b.astype(jnp.float32))


def attention(q, k, v):
    scores = einsum("tgsd,ugd->gstu", q, k) * q.shape[-1] ** -0.5
    token = jnp.arange(q.shape[0])
    scores = jnp.where(token[:, None] >= token, scores, -jnp.inf)
    weights = jax.nn.softmax(scores, -1).astype(jnp.bfloat16)
    return einsum("gstu,ugd->tgsd", weights, v).astype(jnp.bfloat16)


def reference(x, gain, wq, wk, wv, wo):
    a, place = normed(x, gain), jnp.arange(ROWS)
    q = turned(matmul(a, wq).reshape(ROWS, HEADS, HEAD), place, THETA).reshape(ROWS, KV_HEADS, -1, HEAD)
    k = turned(matmul(a, wk).reshape(ROWS, KV_HEADS, HEAD), place, THETA)
    v = matmul(a, wv).reshape(ROWS, KV_HEADS, HEAD)
    seen = attention(q, k, v).reshape(ROWS, HEADS * HEAD)
    return (x.astype(jnp.float32) + jnp.dot(seen, wo, preferred_element_type=jnp.float32)).astype(jnp.bfloat16)
```

```python
import functools

import jax
import jax.numpy as jnp
import numpy as np
from jax import lax
from jax.experimental import pallas as pl
from jax.experimental.pallas import tpu as pltpu
from jax.sharding import PartitionSpec as P

HEAD = 256
HALF = HEAD // 2
THETA = 10000
LOG2E = 1.4426950408889634
HIDDEN = -2e30
N = 16
VMEM = 62 * 2**20
ORDERS = ((2, 4, 8), (4, 8, 2), (8, 2, 4))
ARRIVE = (0, 1, 2, 4, 8, 3, 5, 9, 6, 10, 12, 7, 11, 13, 14, 15)
WKV, WQ0, WQ1, KV, WO0, WO1 = range(6)
EVEN = (2, 4, 8, 6, 10, 12, 14)
ODD = (1, 3, 5, 9, 7, 11, 13, 15)


def _dot(a, b, ca=1, cb=0):
    return lax.dot_general(a, b, (((ca,), (cb,)), ((), ())), preferred_element_type=jnp.float32)


def _cuts(rows):
    big = -(-rows // 3 // 16) * 16
    big = big if rows - 2 * big > 0 else big - 16
    return ((0, big), (big, big), (2 * big, rows - 2 * big))


def _kernel(x_hbm, gain_ref, wq_hbm, wk_hbm, wv_hbm, wo_hbm, near_ref, far_ref, y_hbm,
            x_s, a_s, wkv_s, wq_s, wo_s, kv_s, q_s, mix_s, top_s, seen_s, rot_s, load_sem, store_sem, send_sem, recv_sem):
    me = lax.axis_index("sp")
    bits = {b: lax.rem(lax.div(me, b), 2) for b in (1, 2, 4, 8)}
    steps = {b: b - 2 * b * bit for b, bit in bits.items()}
    other = [me]
    for b in (1, 2, 4, 8):
        other += [o + steps[b] for o in other]
    own, d = x_s.shape
    e = HEAD**-0.5 * LOG2E
    half_cols = d // 2
    group = half_cols // HEAD
    bufs = {
        WKV: (wkv_s, 0, 2 * HEAD, 0), WQ0: (wq_s, 0, half_cols, 1), WQ1: (wq_s, half_cols, half_cols, 2),
        KV: (kv_s, 0, 2 * HEAD, 0), WO0: (wo_s, 0, half_cols, 1), WO1: (wo_s, half_cols, half_cols, 2),
    }

    def copy(c, p, t, to):
        buf, c0, cw, turn = bufs[c]
        r0, rn = _cuts(buf.shape[1])[(p + turn) % 3]
        ref = buf.at[other[t], pl.ds(r0, rn), pl.ds(c0, cw)]
        return pltpu.make_async_remote_copy(
            src_ref=ref, dst_ref=ref, send_sem=send_sem.at[c], recv_sem=recv_sem.at[c, p, t ^ to],
            device_id={"sp": other[to]}, device_id_type=pl.DeviceIdType.MESH)

    def sends(p, t):
        d1, d2, d3 = ORDERS[p]
        return {0: (d1, d2, d3), d1: (d2, d3), d2: (d3,), d1 ^ d2: (d3,)}.get(t, ())

    def start_own(c):
        for i in range(3):
            for p in range(3):
                copy(c, p, 0, sends(p, 0)[i]).start()
        for p in range(3):
            copy(c, p, 0, 1).start()

    def relay(c, *ts):
        for t in ts:
            for p in range(3):
                copy(c, p, t ^ 1, 1).wait_recv()
                if t % 2 == 0:
                    for to in sends(p, t):
                        copy(c, p, t, to).start()
                    copy(c, p, t, 1).start()

    def drain(c):
        buf, c0, cw, _ = bufs[c]
        all_sent = buf.at[pl.ds(0, 15), :, pl.ds(c0, cw)]
        pltpu.make_async_remote_copy(src_ref=all_sent, dst_ref=all_sent, send_sem=send_sem.at[c], recv_sem=recv_sem.at[c, 0, 1],
                                     device_id={"sp": other[1]}, device_id_type=pl.DeviceIdType.MESH).wait_send()

    loads = [
        pltpu.make_async_copy(wk_hbm, wkv_s.at[me, :, pl.ds(0, HEAD)], load_sem.at[0]),
        pltpu.make_async_copy(wv_hbm, wkv_s.at[me, :, pl.ds(HEAD, HEAD)], load_sem.at[1]),
        pltpu.make_async_copy(wq_hbm, wq_s.at[me], load_sem.at[2]),
        pltpu.make_async_copy(x_hbm, x_s, load_sem.at[3]),
        pltpu.make_async_copy(wo_hbm, wo_s.at[me], load_sem.at[4]),
    ]
    for load in loads:
        load.start()
    barrier = pltpu.get_barrier_semaphore()
    for to in (1, 2, 4, 8):
        pl.semaphore_signal(barrier, inc=1, device_id={"sp": other[to]}, device_id_type=pl.DeviceIdType.MESH)
    pl.semaphore_wait(barrier, 4)

    loads[0].wait()
    loads[1].wait()
    start_own(WKV)
    loads[2].wait()
    start_own(WQ0)
    loads[3].wait()

    gain = gain_ref[...].astype(jnp.float32)

    def norm(i, _):
        rows = pl.ds(pl.multiple_of(i * 32, 32), 32)
        wide = x_s[rows, :].astype(jnp.float32)
        scale = lax.rsqrt(jnp.mean(wide * wide, -1, keepdims=True) + 1e-6)
        a_s[rows, :] = (wide * scale * gain).astype(jnp.bfloat16)
        return _

    lax.fori_loop(0, own // 32, norm, 0)
    c0, s0 = far_ref[0, pl.ds(me, 1), :], far_ref[1, pl.ds(me, 1), :]
    rot_s[0] = c0 * near_ref[0] - s0 * near_ref[1]
    rot_s[1] = s0 * near_ref[0] + c0 * near_ref[1]

    def turned(t):
        t = t.astype(jnp.bfloat16).astype(jnp.float32)
        a, b = t[:, :HALF], t[:, HALF:]
        cos, sin = rot_s[0], rot_s[1]
        return jnp.concatenate([a * cos - b * sin, b * cos + a * sin], -1).astype(jnp.bfloat16)

    relay(WKV, 2, 4, 8, 6, 10, 12, 14)
    relay(WQ0, 2, 4, 8)
    relay(WKV, *ODD)
    k = _dot(a_s[...], wkv_s[:, :, :HEAD].reshape(d, HEAD))
    kv_s[me, :, :HEAD] = turned(k)
    v = _dot(a_s[...], wkv_s[:, :, HEAD:].reshape(d, HEAD))
    kv_s[me, :, HEAD:] = v.astype(jnp.bfloat16)
    relay(WQ0, 6, 10, 12, 14)
    start_own(KV)
    relay(WQ0, *ODD)

    def queries(g):
        def one(h, _):
            at = pl.multiple_of(g * half_cols + h * HEAD, HEAD)
            q = _dot(a_s[...], wq_s[:, :, pl.ds(at, HEAD)].reshape(d, HEAD))
            q_s[:, pl.ds(pl.multiple_of(h * own, own), own)] = turned(q).T
            return _

        lax.fori_loop(0, group, one, 0)

    ones = jnp.ones((8, own), jnp.bfloat16)

    def attend(j, first):
        kk = kv_s[j, :, :HEAD]
        values = jnp.concatenate([kv_s[j, :, HEAD:].T, ones], axis=0)
        scores = [_dot(kk, q_s[:, h * own : (h + 1) * own]) for h in range(group)]
        weights, keeps = [], []
        if first:
            ok = lax.broadcasted_iota(jnp.int32, (own, own), 1) >= lax.broadcasted_iota(jnp.int32, (own, own), 0)
        for h, s in enumerate(scores):
            cols = slice(h * own, (h + 1) * own)
            if first:
                s = jnp.where(ok, s, HIDDEN)
                top = s.max(axis=0, keepdims=True)
            else:
                old = top_s[:, cols]
                top = jnp.maximum(old, s.max(axis=0, keepdims=True))
                keeps.append(jnp.exp2((old - top) * e))
            top_s[:, cols] = top
            weights.append(jnp.exp2((s - top) * e).astype(jnp.bfloat16))
        for h, p in enumerate(weights):
            cols = slice(h * own, (h + 1) * own)
            if first:
                mix_s[:, cols] = _dot(values, p)
            else:
                mix_s[:, cols] = mix_s[:, cols] * keeps[h] + _dot(values, p)

    def attention(g, events):
        attend(me, True)

        def step(i, _):
            t = jnp.int32(0)
            for n in range(1, N):
                t = jnp.where(i == n, ARRIVE[n], t)
                if n in events:
                    pl.when(i == n)(events[n])
            j = sum(b * lax.rem(bit + lax.rem(lax.div(t, b), 2), 2) for b, bit in bits.items())
            pl.when(j < me)(lambda: attend(j, False))
            return _

        lax.fori_loop(1, N, step, 0)

        for h in range(group):
            cols = slice(h * own, (h + 1) * own)
            out = mix_s[:HEAD, cols] * (1 / mix_s[HEAD : HEAD + 1, cols])
            at = g * half_cols + h * HEAD
            seen_s[:, at : at + HEAD] = out.T.astype(jnp.bfloat16)

    def do(*acts):
        def run():
            for act, *args in acts:
                act(*args)
        return run

    queries(0)
    first_events = {n: [(relay, KV, ARRIVE[n])] for n in range(1, N)}
    first_events[1] += [(start_own, WQ1)]
    first_events[5] += [(relay, WQ1, 2)]
    first_events[6] += [(relay, WQ1, 4)]
    first_events[7] += [(relay, WQ1, 8)]
    first_events[8] += [(loads[4].wait,), (start_own, WO0)]
    first_events[9] += [(relay, WQ1, 6)]
    first_events[10] += [(relay, WQ1, 10)]
    first_events[11] += [(relay, WQ1, 12)]
    first_events[12] += [(relay, WQ1, 14)]
    first_events[14] += [(start_own, WO1)]
    first_events[15] += [(relay, WQ1, *ODD)]
    attention(0, {n: do(*acts) for n, acts in first_events.items()})
    queries(1)
    second_events = {1: [(relay, WO0, 2)], 2: [(relay, WO0, 4)], 3: [(relay, WO0, 8)], 4: [(relay, WO1, 2)], 5: [(relay, WO1, 4)],
                     6: [(relay, WO1, 8)], 7: [(relay, WO0, 6)], 8: [(relay, WO0, 10)], 9: [(relay, WO0, 12)], 10: [(relay, WO0, 14)],
                     11: [(relay, WO1, 6)], 12: [(relay, WO1, 10)], 13: [(relay, WO1, 12)], 14: [(relay, WO1, 14)]}
    attention(1, {n: do(*acts) for n, acts in second_events.items()})

    def project(g):
        def one(n, _):
            cols = pl.ds(pl.multiple_of(g * half_cols + n * HEAD, HEAD), HEAD)
            y = _dot(seen_s[...], wo_s[:, :, cols].reshape(d, HEAD))
            x_s[:, cols] = (x_s[:, cols].astype(jnp.float32) + y).astype(jnp.bfloat16)
            return _

        lax.fori_loop(0, group, one, 0)
        cols = pl.ds(g * half_cols, half_cols)
        out = pltpu.make_async_copy(x_s.at[:, cols], y_hbm.at[:, cols], store_sem.at[g])
        out.start()
        return out

    relay(WO0, *ODD)
    out0 = project(0)
    relay(WO1, *ODD)
    out1 = project(1)
    for c in range(6):
        drain(c)
    out0.wait()
    out1.wait()


def _angles(own):
    turn = THETA ** (-np.arange(HALF) / HALF)
    table = lambda place: np.stack([np.cos(place[:, None] * turn), np.sin(place[:, None] * turn)]).astype(np.float32)
    return table(np.arange(own)), table(np.arange(N) * own)


def solution(mesh):
    def step(x, gain, wq, wk, wv, wo):
        own, d = x.shape
        bf, f32 = jnp.bfloat16, jnp.float32
        near, far = _angles(own)
        anywhere, vmem = pl.BlockSpec(memory_space=pl.ANY), pl.BlockSpec(memory_space=pltpu.VMEM)
        rows = wq.shape[0]
        cols = d // 2 // HEAD * own
        return pl.pallas_call(
            _kernel,
            out_shape=jax.ShapeDtypeStruct((own, d), bf),
            in_specs=[anywhere, vmem, anywhere, anywhere, anywhere, anywhere, vmem, vmem],
            out_specs=anywhere,
            scratch_shapes=[
                pltpu.VMEM((own, d), bf), pltpu.VMEM((own, d), bf),
                pltpu.VMEM((N, rows, 2 * HEAD), bf), pltpu.VMEM((N, rows, d), bf), pltpu.VMEM((N, rows, d), bf),
                pltpu.VMEM((N, own, 2 * HEAD), bf),
                pltpu.VMEM((HEAD, cols), bf), pltpu.VMEM((HEAD + 8, cols), f32), pltpu.VMEM((1, cols), f32),
                pltpu.VMEM((own, d), bf), pltpu.VMEM((2, own, HALF), f32),
                pltpu.SemaphoreType.DMA((5,)), pltpu.SemaphoreType.DMA((2,)),
                pltpu.SemaphoreType.DMA((6,)), pltpu.SemaphoreType.DMA((6, 3, N)),
            ],
            compiler_params=pltpu.CompilerParams(collective_id=0, has_side_effects=True, vmem_limit_bytes=VMEM),
            cost_estimate=pl.CostEstimate(flops=50 * 10**9, bytes_accessed=10**7, transcendentals=10**7),
        )(x, gain.reshape(1, d), wq, wk, wv, wo, jnp.asarray(near), jnp.asarray(far))

    tokens, whole = P(("dp", "sp"), None), P("sp", None)
    return jax.shard_map(
        step,
        mesh=mesh,
        in_specs=(tokens, P(None), whole, whole, whole, whole),
        out_specs=tokens,
        check_vma=False,
    )
```
